32 devices in a mesh: mem: 16 (over z, x, core), space: 2 (over y).
Axes of the slice: x: 2, y: 2, z: 4, core: 2. Of those that a mesh axis runs over, the one named last changes fastest.
Arguments:
- prior_sample_set: float32 [512, 64, 128], P('mem', 'space'), may hold values from -6 to 6
- perturbed_obs: float32 [512, 64, 128], P('mem', 'space'), may hold values from -6 to 6
- measured_slot_table: int32 [64, 128], P('space'), may hold values from 0 to 127
- obs_var: float32 [64, 128], P('space'), may hold values from 0.25 to 2
- neighbours: int32 [64, 2], P('space'), may hold values from 0 to 63, as said below
- norm_gain: float32 [64], replicated, may hold values from 0.5 to 1.5
- w_in: bfloat16 [64, 512], replicated, may hold values from -0.75 to 0.75
- b_in: float32 [512], replicated, may hold values from -3 to 3
- w_out: bfloat16 [512, 64], replicated, may hold values from -0.25 to 0.25
- b_out: float32 [64], replicated, may hold values from -1.2 to 1.2
Outputs:
- analysis: float32 [512, 64, 128], P('mem', 'space')
The draws below stay inside these ranges and needn't reach their ends.
Inputs may be any that keep to these rules, and one draw needn't show every extreme that they name: `neighbours`: row p names 2 different blocks among p - 1, p, p + 1 taken modulo 64, in the order of these offsets. `measured_slot_table`: entry [b, j] names a variable of patch b.
All inputs are finite; a program needn't handle non-finite values.
Results may differ from the reference program's by a relative error of at most 0.0026.
Values sent between devices are 32-bit elements; how exact they have to be, the bound alone decides.
A program may use at most 64 MiB of HBM per device.

```python
import math
import jax
import jax.numpy as jnp
from jax import lax

LEV = 64
HID = 512
OB = 128
PREDICTION_HOPS = 2
PV = 128
M = 512
NPATCH = 64


def draw_neighbours(key, part):
    dropped = jax.random.randint(key, (NPATCH,), 0, 3)
    first_offset = jnp.where(dropped == 0, 0, -1)
    second_offset = jnp.where(dropped == 2, 0, 1)
    base = jnp.arange(NPATCH, dtype=jnp.int32)
    offsets = jnp.stack([first_offset, second_offset], axis=1).astype(jnp.int32)
    return ((base[:, None] + offsets) % NPATCH).astype(jnp.int32)


def set_ends(entries, key, least, high):
    extent = entries.shape
    spot = [jax.random.randint(jax.random.fold_in(key, axis), (), 0, extent[axis]) for axis in range(len(extent))]
    entries = entries.at[tuple(spot)].set(least)
    longest = extent.index(max(extent))
    spot[longest] = (spot[longest] + 1) % extent[longest]
    return entries.at[tuple(spot)].set(high)


def block_scale(own_key, extent, pieces, least, high):
    gain = 1.0
    for dim, parts in pieces:
        draws = jax.random.uniform(jax.random.fold_in(jax.random.fold_in(own_key, 6), dim), (parts,), jnp.float32, least / len(pieces), high / len(pieces))
        gain = gain * jnp.repeat(jnp.exp(draws), extent[dim] // parts).reshape((-1,) + (1,) * (len(extent) - 1 - dim))
    return gain


def scatter_about(rng, shape, scale, bound, cuts=(), kind=jnp.bfloat16):
    loudness = block_scale(rng, shape, cuts, -0.22, 0.18) if cuts else 1.0
    values = jax.random.normal(rng, shape, jnp.float32) * scale * loudness
    return jnp.minimum(jnp.maximum(values, -bound), bound).astype(kind)


def setup_inputs(seed: int = 0) -> dict:
    key_of = jax.random.split(jax.random.key(seed), 11)
    prior_sample_set = scatter_about(key_of[0], (M, NPATCH, PV), 1.0, 6.0, ((0, 16), (1, 2)), jnp.float32)
    perturbed_obs = scatter_about(key_of[1], (M, NPATCH, OB), 1.0, 6.0, ((0, 16), (1, 2)), jnp.float32)
    measured_slot_table = set_ends(jax.random.randint(key_of[2], (NPATCH, OB), 0, PV), jax.random.fold_in(key_of[2], 1), 0, PV - 1).astype(jnp.int32)
    obs_var = jnp.clip(jnp.exp(math.log(2.0) - 2.0794415 * jax.random.uniform(key_of[3], (NPATCH, OB), jnp.float32) ** block_scale(key_of[3], (NPATCH, OB), ((0, 2),), -0.2, 0.2)), 0.25, 2.0)
    neighbours = draw_neighbours(jax.random.fold_in(key_of[10], 71), 0)
    norm_gain = jnp.clip(1.0 + 0.1 * jax.random.normal(key_of[5], (LEV,), jnp.float32), 0.5, 1.5)
    w_in = scatter_about(key_of[6], (LEV, HID), LEV ** -0.5, 0.75)
    b_in = scatter_about(key_of[7], (HID,), 0.5, 3.0, (), jnp.float32)
    w_out = scatter_about(key_of[8], (HID, LEV), HID ** -0.5, 0.25)
    b_out = scatter_about(key_of[9], (LEV,), 0.2, 1.2, (), jnp.float32)
    return {"prior_sample_set": prior_sample_set, "perturbed_obs": perturbed_obs, "measured_slot_table": measured_slot_table, "obs_var": obs_var, "neighbours": neighbours, "norm_gain": norm_gain, "w_in": w_in, "b_in": b_in, "w_out": w_out, "b_out": b_out}


def advance(profile_total, norm_gain, w_in, b_in, w_out, b_out):
    for propagate_once in range(PREDICTION_HOPS):
        inverse = lax.rsqrt(lax.optimization_barrier(jnp.mean(profile_total * profile_total, axis=-1, keepdims=True)) + 1e-06)
        normed = (profile_total * inverse * norm_gain).astype(jnp.bfloat16)
        hidden = jax.nn.silu(jnp.dot(normed.astype(jnp.float32), w_in.astype(jnp.float32), preferred_element_type=jnp.float32) + b_in).astype(jnp.bfloat16)
        profile_total = profile_total + jnp.dot(hidden.astype(jnp.float32), w_out.astype(jnp.float32), preferred_element_type=jnp.float32) + b_out
    return profile_total

def update(members, measurement_readings, innovation):
    ensemble_size = members.shape[0]
    anomaly = members - lax.optimization_barrier(jnp.mean(members, axis=0))
    spread = measurement_readings - lax.optimization_barrier(jnp.mean(measurement_readings, axis=0))
    covariance = jnp.dot(spread.T, spread, precision=lax.Precision.HIGHEST) / (ensemble_size - 1)
    covariance = covariance + jnp.eye(measurement_readings.shape[1], dtype=covariance.dtype)
    factor = jnp.linalg.cholesky(covariance)
    partial_solve = lax.linalg.triangular_solve(factor, innovation.T, left_side=True, lower=True)
    weights = lax.linalg.triangular_solve(factor, partial_solve, left_side=True, lower=True, transpose_a=True)
    cross_cov = jnp.dot(anomaly.T, spread, precision=lax.Precision.HIGHEST) / (ensemble_size - 1)
    return members + jnp.dot(cross_cov, weights, precision=lax.Precision.HIGHEST).T

def solve_batch(members, measurement_readings, innovation):
    return jax.vmap(update, in_axes=(1, 1, 1), out_axes=1)(members, measurement_readings, innovation)

def split_pair(picked):
    block_width = picked.shape[-1] // 2
    measurement_readings = picked[..., :block_width].reshape(picked.shape[0], picked.shape[1], -1)
    innovation = picked[..., block_width:].reshape(picked.shape[0], picked.shape[1], -1)
    return (measurement_readings, innovation)

def reference(prior_sample_set, perturbed_obs, measured_slot_table, obs_var, neighbours, norm_gain, w_in, b_in, w_out, b_out):
    profile_total = prior_sample_set.reshape(-1, LEV)
    row_total = profile_total.shape[0]
    block_rows = math.gcd(row_total, 8192)
    stacked = profile_total.reshape(row_total // block_rows, block_rows, LEV)
    propagated_vector = lax.map(lambda piece: advance(piece, norm_gain, w_in, b_in, w_out, b_out), stacked)
    propagate_model_grid = propagated_vector.reshape(prior_sample_set.shape)
    measurement_readings = jnp.take_along_axis(propagate_model_grid, measured_slot_table[None], axis=2)
    weight_root = lax.rsqrt(obs_var)[None]
    paired = jnp.concatenate([measurement_readings * weight_root, (perturbed_obs - measurement_readings) * weight_root], axis=-1)
    batch_sample_total = math.gcd(NPATCH, 8)

    def solve_group(starting_position):
        rows_here = lax.dynamic_slice_in_dim(neighbours, starting_position, batch_sample_total, 0)
        picked = paired[:, rows_here]
        observed_here, innovation_here = split_pair(picked)
        nearby_samples = lax.dynamic_slice_in_dim(propagate_model_grid, starting_position, batch_sample_total, 1)
        return solve_batch(nearby_samples, observed_here, innovation_here)
    firsts = jnp.arange(NPATCH // batch_sample_total, dtype=jnp.int32) * batch_sample_total
    solved = lax.map(solve_group, firsts)
    return jnp.transpose(solved, (1, 0, 2, 3)).reshape(prior_sample_set.shape)
```

```python
import functools
import jax
import jax.numpy as jnp
from jax import lax
from jax.experimental import pallas as pl
from jax.experimental.pallas import tpu as pltpu
from jax.sharding import PartitionSpec as P

LEV = 64
HOPS = 2
F32 = jnp.float32
BF16 = jnp.bfloat16
MESH = pl.DeviceIdType.MESH


def dot1(a, b):
    return jnp.dot(a, b, preferred_element_type=F32)


def split(a):
    hi = a.astype(BF16)
    return hi, (a - hi.astype(F32)).astype(BF16)


def dot3(a, b):
    ah, al = split(a)
    bh, bl = split(b)
    return dot1(ah, bh) + dot1(ah, bl) + dot1(al, bh)


def doth(a, b):
    return jnp.dot(a, b, preferred_element_type=F32, precision=lax.Precision.HIGHEST)


def spread_row(v, r):
    return jnp.broadcast_to(v[r:r + 1, :], v.shape)

def sweep(p, base, rows, lanes):
    cols = [jnp.broadcast_to(p[:, base + j:base + j + 1], p.shape) for j in range(8)]
    for j in range(0, 8, 2):
        ca, cb = cols[j], cols[j + 1]
        al, be, de = spread_row(ca, j), spread_row(cb, j), spread_row(cb, j + 1)
        inv = 1.0 / (al * de - be * be)
        ra, rb = rows == j, rows == j + 1
        na = jnp.where(ra, -1.0, jnp.where(rb, 0.0, ca))
        nb = jnp.where(rb, -1.0, jnp.where(ra, 0.0, cb))

        def step(v, a, b):
            t = na * (de * a - be * b) + nb * (al * b - be * a)
            return jnp.where(ra | rb, 0.0, v) - t * inv

        for i in range(j + 2, 8):
            cols[i] = step(cols[i], spread_row(cols[i], j), spread_row(cols[i], j + 1))
        la, lb = lanes == base + j, lanes == base + j + 1
        a = jnp.where(la, 1.0, jnp.where(lb, 0.0, spread_row(p, j)))
        b = jnp.where(lb, 1.0, jnp.where(la, 0.0, spread_row(p, j + 1)))
        p = step(jnp.where(la | lb, 0.0, p), a, b)
    return p

def inverses(mats, nb=16):
    size = mats[0].shape[0]
    rows = lax.broadcasted_iota(jnp.int32, (8, size), 0)
    lanes = lax.broadcasted_iota(jnp.int32, (8, size), 1)
    wide = lax.broadcasted_iota(jnp.int32, (size, size), 1)
    mats = list(mats)
    for lo in range(0, size, nb):
        panels = [[a[lo + q:lo + q + 8] for q in range(0, nb, 8)] for a in mats]
        for q in range(nb // 8):
            base = lo + 8 * q
            here = (lanes >= base) & (lanes < base + 8)
            for m in panels:
                m[q] = sweep(m[q], base, rows, lanes)
            for m in panels:
                for i in range(nb // 8):
                    if i != q:
                        acc = jnp.where(here, 0.0, m[i])
                        for j in range(8):
                            acc = acc - m[i][:, base + j:base + j + 1] * m[q][j:j + 1, :]
                        m[i] = acc
        hole = (wide >= lo) & (wide < lo + nb)
        for k, a in enumerate(mats):
            p = jnp.concatenate(panels[k], axis=0)
            parts = [p]
            if lo: parts.insert(0, jnp.zeros((lo, size), F32))
            if lo + nb < size: parts.append(jnp.zeros((size - lo - nb, size), F32))
            pad = jnp.concatenate(parts, axis=0)
            out = [p]
            if lo:
                t = a[:lo]
                out.insert(0, jnp.where(hole[:lo], 0.0, t) - doth(t, pad))
            if lo + nb < size:
                t = a[lo + nb:]
                out.append(jnp.where(hole[lo + nb:], 0.0, t) - doth(t, pad))
            mats[k] = jnp.concatenate(out, axis=0)
    return mats


def kernel(n, ns, prior, pert, slot, var, nbr, gain, w_in, b_in, w_out, b_out, out,
           xb, pb, yb, ib, res, w1, w2,
           xs, xr, ps, pr, ys, yr, isd, ir, os_, orr, loc):
    me = lax.axis_index("mem")
    sp = lax.axis_index("space")
    count = xb.shape[0]
    size = xb.shape[1]
    width = xb.shape[2]
    each = size // n
    gs = 4 if n % 4 == 0 else 1
    groups = n // gs
    grows = gs * each
    hid = w_in.shape[1]
    span = n * count
    total = span * ns
    my_group = me // gs

    def window(m, p):
        w = m
        if gs == 4:
            z = m // 4
            w = z * 4 + lax.rem(lax.rem(m // 2, 2) + z, 2) * 2 + lax.rem(m, 2)
        return jnp.where(lax.rem(p, 2) == 0, w, n - 1 - w)

    def holder(w, p):
        w = jnp.where(lax.rem(p, 2) == 0, w, n - 1 - w)
        if gs == 1:
            return w
        z = w // 4
        return z * 4 + lax.rem(lax.rem(w // 2, 2) + z, 2) * 2 + lax.rem(w, 2)

    win = window(me, sp)
    first = win * count
    rsp = lax.rem(sp + (win + 1) // n, ns)
    lsp = lax.rem(sp + ns - (n - win) // n, ns)
    right = (holder(lax.rem(win + 1, n), rsp), rsp)
    left = (holder(lax.rem(win + n - 1, n), lsp), lsp)

    def partner(i):
        g = lax.rem(my_group + groups - i // gs, groups)
        return g * gs + lax.rem(me + lax.rem(i, gs), gs)

    bar = pltpu.get_barrier_semaphore()

    @pl.loop(1, n)
    def _(k):
        pl.semaphore_signal(bar, inc=1, device_id=(lax.rem(me + k, n), sp), device_id_type=MESH)

    pl.semaphore_signal(bar, inc=1, device_id=left, device_id_type=MESH)
    pl.semaphore_signal(bar, inc=1, device_id=right, device_id_type=MESH)
    pl.semaphore_wait(bar, n + 1)

    def mine(i):
        return pl.ds(pl.multiple_of(i * each, each), each)

    def fwd(src, dst, ss, rs, d):
        return pltpu.make_async_remote_copy(
            src_ref=src.at[pl.ds(window(d, sp) * count, count)], dst_ref=dst.at[:, mine(me), :],
            send_sem=ss.at[d], recv_sem=rs.at[me], device_id=(d, sp), device_id_type=MESH)

    def arrived(src, dst, ss, rs, s):
        return pltpu.make_async_remote_copy(
            src_ref=src.at[pl.ds(window(s, sp) * count, count)], dst_ref=dst.at[:, mine(s), :],
            send_sem=ss.at[s], recv_sem=rs.at[s], device_id=(s, sp), device_id_type=MESH)

    def own(src, dst, i):
        return pltpu.make_async_copy(src.at[pl.ds(first, count)], dst.at[:, mine(me), :], loc.at[i])

    @pl.loop(1, n)
    def _(k):
        fwd(prior, xb, xs, xr, partner(k)).start()

    own(prior, xb, 0).start()
    own(pert, pb, 1).start()

    zero = jnp.zeros((LEV, hid), BF16)
    half = (w_in[...].astype(F32) * 0.5).astype(BF16)
    w1[:LEV, :hid] = half
    w1[:LEV, hid:] = zero
    w1[LEV:, :hid] = zero
    w1[LEV:, hid:] = half
    w2[:LEV, :hid] = w_out[...]
    w2[:LEV, hid:] = zero
    w2[LEV:, :hid] = zero
    w2[LEV:, hid:] = w_out[...]
    gain2 = jnp.concatenate([gain[...], gain[...]], axis=1)
    bi = b_in[...] * 0.5
    bi2 = jnp.concatenate([bi, bi], axis=1)
    bo2 = jnp.concatenate([b_out[...], b_out[...]], axis=1)
    ri = lax.broadcasted_iota(jnp.int32, (width, width), 0)
    ci = lax.broadcasted_iota(jnp.int32, (width, width), 1)
    ones = jnp.where((ri < LEV) == (ci < LEV), 1.0 / LEV, 0.0).astype(BF16)
    hots = [jnp.where(slot[pl.ds(first + c, 1), :] == ri, 1.0, 0.0).astype(BF16) for c in range(count)]
    roots = [lax.rsqrt(var[pl.ds(first + c, 1), :]) for c in range(count)]

    own(prior, xb, 0).wait()

    def halo(buf, rows, ss, rs, g, side):
        if side == 0:
            return pltpu.make_async_remote_copy(
                src_ref=buf.at[count, rows, :], dst_ref=buf.at[0, rows, :],
                send_sem=ss.at[0, g], recv_sem=rs.at[0, g], device_id=right, device_id_type=MESH)
        return pltpu.make_async_remote_copy(
            src_ref=buf.at[1, rows, :], dst_ref=buf.at[count + 1, rows, :],
            send_sem=ss.at[1, g], recv_sem=rs.at[1, g], device_id=left, device_id_type=MESH)

    def group_rows(g):
        return pl.ds(pl.multiple_of(g * grows, grows), grows)

    @pl.loop(0, groups)
    def _(t):
        g = lax.rem(my_group + t, groups)
        for q in range(gs):
            s = g * gs + q

            @pl.when(s != me)
            def _():
                arrived(prior, xb, xs, xr, s).wait_recv()

        rows = group_rows(g)
        x = xb[:, rows, :].reshape(count * grows, width)
        for _ in range(HOPS):
            hi, lo = split(x * x)
            inv = lax.rsqrt(dot1(hi, ones) + dot1(lo, ones) + 1e-6)
            normed = (x * inv * gain2).astype(BF16)
            h = dot1(normed, w1[...]) + bi2
            hidden = (h + h * jnp.tanh(h)).astype(BF16)
            x = x + lax.dot_general(hidden, w2[...], (((1,), (1,)), ((), ())), preferred_element_type=F32) + bo2
        x = x.reshape(count, grows, width)
        xb[:, rows, :] = x
        for c in range(count):
            hi, lo = split(x[c])
            yb[c + 1, rows, :] = (dot1(hi, hots[c]) + dot1(lo, hots[c])) * roots[c]
        halo(yb, rows, ys, yr, g, 0).start()
        halo(yb, rows, ys, yr, g, 1).start()

    @pl.loop(1, n)
    def _(k):
        fwd(pert, pb, ps, pr, partner(k)).start()

    @pl.loop(0, groups)
    def _(g):
        for side in range(2):
            halo(yb, group_rows(g), ys, yr, g, side).wait_recv()

    def pick(buf, c, rows, length):
        row = first + c
        patch = sp * span + row
        pair = nbr[pl.ds(row, 1), :]
        a = jnp.broadcast_to(pair[:, 0:1], (length, width)) == lax.rem(patch + total - 1, total)
        b = jnp.broadcast_to(pair[:, 1:2], (length, width)) == lax.rem(patch + 1, total)
        mid = buf[c + 1, rows, :]
        return jnp.concatenate(
            [jnp.where(a, buf[c, rows, :], mid), jnp.where(b, buf[c + 2, rows, :], mid)], axis=1)

    every = pl.ds(0, size)
    grams = []
    for c in range(count):
        y = pick(yb, c, every, size)
        bb = y - jnp.mean(y, axis=0, keepdims=True)
        x = xb[c]
        z = jnp.concatenate([bb, x - jnp.mean(x, axis=0, keepdims=True)], axis=1)
        grams.append(dot3(bb.T, z) * (1.0 / (size - 1)))
    eye = jnp.where(ri == ci, 1.0, 0.0)
    w = width
    pinv = inverses([m[:w, :w] + eye for m in grams])

    own(pert, pb, 1).wait()

    @pl.loop(0, groups)
    def _(t):
        g = lax.rem(my_group + t, groups)
        for q in range(gs):
            s = g * gs + q

            @pl.when(s != me)
            def _():
                arrived(pert, pb, ps, pr, s).wait_recv()

        rows = group_rows(g)
        for c in range(count):
            ib[c + 1, rows, :] = pb[c, rows, :] * roots[c] - yb[c + 1, rows, :]
        halo(ib, rows, isd, ir, g, 0).start()
        halo(ib, rows, isd, ir, g, 1).start()

    es = [doth(pinv[c], grams[c][:w, w:2 * w]) for c in range(count)]
    ts = [grams[c][w:, w:2 * w] + eye - doth(grams[c][w:, :w], es[c]) for c in range(count)]
    fs = [doth(pinv[c], grams[c][:w, 2 * w:]) for c in range(count)]
    tinv = inverses(ts)
    gains = []
    for c in range(count):
        k2 = doth(tinv[c], grams[c][w:, 2 * w:] - doth(grams[c][w:, :w], fs[c]))
        k1 = fs[c] - doth(es[c], k2)
        gains.append(jnp.concatenate([k1, k2], axis=0))

    def back(d):
        return pltpu.make_async_remote_copy(
            src_ref=res.at[:, mine(d), :], dst_ref=out.at[pl.ds(first, count)],
            send_sem=os_.at[d], recv_sem=orr.at[me], device_id=(d, sp), device_id_type=MESH)

    def returned(s):
        return pltpu.make_async_remote_copy(
            src_ref=res.at[:, mine(s), :], dst_ref=out.at[pl.ds(window(s, sp) * count, count)],
            send_sem=os_.at[s], recv_sem=orr.at[s], device_id=(s, sp), device_id_type=MESH)

    gh = [split(m) for m in gains]

    @pl.loop(0, groups)
    def _(t):
        g = lax.rem(my_group + groups // 2 + t, groups)
        rows = group_rows(g)
        for side in range(2):
            halo(ib, rows, isd, ir, g, side).wait_recv()
        for c in range(count):
            ih, il = split(pick(ib, c, rows, grows))
            res[c, rows, :] = xb[c, rows, :] + dot1(ih, gh[c][0]) + dot1(ih, gh[c][1]) + dot1(il, gh[c][0])
        for q in range(gs):
            d = g * gs + lax.rem(me + q, gs)

            @pl.when(d != me)
            def _():
                back(d).start()

    last = pltpu.make_async_copy(res.at[:, mine(me), :], out.at[pl.ds(first, count)], loc.at[2])
    last.start()

    @pl.loop(0, groups)
    def _(g):
        for side in range(2):
            halo(yb, group_rows(g), ys, yr, g, side).wait_send()
            halo(ib, group_rows(g), isd, ir, g, side).wait_send()

    last.wait()

    @pl.loop(1, n)
    def _(k):
        d = lax.rem(me + k, n)
        fwd(prior, xb, xs, xr, d).wait_send()
        fwd(pert, pb, ps, pr, d).wait_send()
        back(d).wait_send()
        returned(d).wait_recv()


def body(prior, pert, slot, var, nbr, gain, w_in, b_in, w_out, b_out):
    n = lax.axis_size("mem")
    ns = lax.axis_size("space")
    each, span, width = prior.shape
    count = span // n
    size = each * n
    hid = w_in.shape[1]
    vm = pl.BlockSpec(memory_space=pltpu.VMEM)
    anyw = pl.BlockSpec(memory_space=pl.ANY)
    groups = n // (4 if n % 4 == 0 else 1)
    dma = pltpu.SemaphoreType.DMA
    out = pl.pallas_call(
        functools.partial(kernel, n, ns),
        out_shape=jax.ShapeDtypeStruct((span, each, width), F32),
        in_specs=[anyw, anyw, vm, vm, vm, vm, vm, vm, vm, vm],
        out_specs=anyw,
        scratch_shapes=[
            pltpu.VMEM((count, size, width), F32),
            pltpu.VMEM((count, size, width), F32),
            pltpu.VMEM((count + 2, size, width), F32),
            pltpu.VMEM((count + 2, size, width), F32),
            pltpu.VMEM((count, size, width), F32),
            pltpu.VMEM((width, 2 * hid), BF16),
            pltpu.VMEM((width, 2 * hid), BF16),
            dma((n,)), dma((n,)), dma((n,)), dma((n,)),
            dma((2, groups)), dma((2, groups)), dma((2, groups)), dma((2, groups)),
            dma((n,)), dma((n,)), dma((3,)),
        ],
        compiler_params=pltpu.CompilerParams(
            collective_id=0, has_side_effects=True, vmem_limit_bytes=48 * 1024 * 1024),
        name="cycle",
    )(jnp.transpose(prior, (1, 0, 2)), jnp.transpose(pert, (1, 0, 2)), slot, var, nbr,
      gain[None], w_in, b_in[None], w_out.T, b_out[None])
    return jnp.transpose(out, (1, 0, 2))


def solution(mesh):
    in_specs = (
        P("mem", "space", None), P("mem", "space", None),
        P("space", None), P("space", None), P("space", None),
        P(), P(), P(), P(), P(),
    )
    return jax.shard_map(body, mesh=mesh, in_specs=in_specs, out_specs=P("mem", "space", None), check_vma=False)
```

```python
import functools
import jax
import jax.numpy as jnp
from jax import lax
from jax.experimental import pallas as pl
from jax.experimental.pallas import tpu as pltpu
from jax.sharding import PartitionSpec as P

LEV = 64
HOPS = 2
F32 = jnp.float32
BF16 = jnp.bfloat16
MESH = pl.DeviceIdType.MESH


def dot1(a, b):
    return jnp.dot(a, b, preferred_element_type=F32)


def split(a):
    hi = a.astype(BF16)
    return hi, (a - hi.astype(F32)).astype(BF16)


def doth(a, b):
    return jnp.dot(a, b, preferred_element_type=F32, precision=lax.Precision.HIGHEST)


def spread_row(v, r):
    return jnp.broadcast_to(v[r:r + 1, :], v.shape)

def sweep(p, base, rows, lanes):
    cols = [jnp.broadcast_to(p[:, base + j:base + j + 1], p.shape) for j in range(8)]
    for j in range(0, 8, 2):
        ca, cb = cols[j], cols[j + 1]
        al, be, de = spread_row(ca, j), spread_row(cb, j), spread_row(cb, j + 1)
        inv = 1.0 / (al * de - be * be)
        ra, rb = rows == j, rows == j + 1
        na = jnp.where(ra, -1.0, jnp.where(rb, 0.0, ca))
        nb = jnp.where(rb, -1.0, jnp.where(ra, 0.0, cb))

        def step(v, a, b):
            t = na * (de * a - be * b) + nb * (al * b - be * a)
            return jnp.where(ra | rb, 0.0, v) - t * inv

        for i in range(j + 2, 8):
            cols[i] = step(cols[i], spread_row(cols[i], j), spread_row(cols[i], j + 1))
        la, lb = lanes == base + j, lanes == base + j + 1
        a = jnp.where(la, 1.0, jnp.where(lb, 0.0, spread_row(p, j)))
        b = jnp.where(lb, 1.0, jnp.where(la, 0.0, spread_row(p, j + 1)))
        p = step(jnp.where(la | lb, 0.0, p), a, b)
    return p

def inverses(mats, nb=16):
    size = mats[0].shape[0]
    rows = lax.broadcasted_iota(jnp.int32, (8, size), 0)
    lanes = lax.broadcasted_iota(jnp.int32, (8, size), 1)
    wide = lax.broadcasted_iota(jnp.int32, (size, size), 1)
    mats = list(mats)
    for lo in range(0, size, nb):
        panels = [[a[lo + q:lo + q + 8] for q in range(0, nb, 8)] for a in mats]
        for q in range(nb // 8):
            base = lo + 8 * q
            here = (lanes >= base) & (lanes < base + 8)
            for m in panels:
                m[q] = sweep(m[q], base, rows, lanes)
            for m in panels:
                for i in range(nb // 8):
                    if i != q:
                        acc = jnp.where(here, 0.0, m[i])
                        for j in range(8):
                            acc = acc - m[i][:, base + j:base + j + 1] * m[q][j:j + 1, :]
                        m[i] = acc
        hole = (wide >= lo) & (wide < lo + nb)
        for k, a in enumerate(mats):
            p = jnp.concatenate(panels[k], axis=0)
            parts = [p]
            if lo: parts.insert(0, jnp.zeros((lo, size), F32))
            if lo + nb < size: parts.append(jnp.zeros((size - lo - nb, size), F32))
            pad = jnp.concatenate(parts, axis=0)
            out = [p]
            if lo:
                t = a[:lo]
                out.insert(0, jnp.where(hole[:lo], 0.0, t) - doth(t, pad))
            if lo + nb < size:
                t = a[lo + nb:]
                out.append(jnp.where(hole[lo + nb:], 0.0, t) - doth(t, pad))
            mats[k] = jnp.concatenate(out, axis=0)
    return mats


def kernel(n, ns, prior_in, pert_in, *refs):
    small_in, refs = refs[:8], refs[8:]
    out, raw, rawp, prior, pert = refs[:5]
    slot, var, nbr, gain, w_in, b_in, w_out, b_out = small = refs[5:13]
    (xb, pb, yb, ib, res, w1, w2,
     xs, xr, ps, pr, ys, yr, isd, ir, os_, orr, loc) = refs[13:]
    me = lax.axis_index("mem")
    sp = lax.axis_index("space")
    count = xb.shape[0]
    size = xb.shape[1]
    width = xb.shape[2]
    each = size // n
    gs = 4 if n % 4 == 0 else 1
    groups = n // gs
    grows = gs * each
    hid = w_in.shape[1]
    span = n * count
    total = span * ns
    my_group = me // gs

    def window(m, p):
        w = m
        if gs == 4:
            z = m // 4
            w = z * 4 + lax.rem(lax.rem(m // 2, 2) + z, 2) * 2 + lax.rem(m, 2)
        return jnp.where(lax.rem(p, 2) == 0, w, n - 1 - w)

    def holder(w, p):
        w = jnp.where(lax.rem(p, 2) == 0, w, n - 1 - w)
        if gs == 1:
            return w
        z = w // 4
        return z * 4 + lax.rem(lax.rem(w // 2, 2) + z, 2) * 2 + lax.rem(w, 2)

    win = window(me, sp)
    first = win * count
    rsp = lax.rem(sp + (win + 1) // n, ns)
    lsp = lax.rem(sp + ns - (n - win) // n, ns)
    right = (holder(lax.rem(win + 1, n), rsp), rsp)
    left = (holder(lax.rem(win + n - 1, n), lsp), lsp)

    def partner(i):
        g = lax.rem(my_group + groups - i // gs, groups)
        return g * gs + lax.rem(me + lax.rem(i, gs), gs)

    loads = [pltpu.make_async_copy(prior_in, raw, loc.at[0]), pltpu.make_async_copy(pert_in, rawp, loc.at[1])]
    loads += [pltpu.make_async_copy(a, b, loc.at[3 + i]) for i, (a, b) in enumerate(zip(small_in, small))]
    for load in loads:
        load.start()

    bar = pltpu.get_barrier_semaphore()

    @pl.loop(1, n)
    def _(k):
        pl.semaphore_signal(bar, inc=1, device_id=(lax.rem(me + k, n), sp), device_id_type=MESH)

    pl.semaphore_signal(bar, inc=1, device_id=left, device_id_type=MESH)
    pl.semaphore_signal(bar, inc=1, device_id=right, device_id_type=MESH)

    def mine(i):
        return pl.ds(pl.multiple_of(i * each, each), each)

    def by_patch(src, dst):
        @pl.loop(0, span)
        def _(p):
            for m in range(0, each, 8):
                dst[p, pl.ds(m, 8), :] = src[pl.ds(p + m * span, 8, stride=span), :]

    def keep(src, dst):
        for c in range(count):
            dst[c, mine(me), :] = src[first + c]

    loads[0].wait()
    by_patch(raw, prior)
    pl.semaphore_wait(bar, n + 1)

    def fwd(src, dst, ss, rs, d):
        return pltpu.make_async_remote_copy(
            src_ref=src.at[pl.ds(window(d, sp) * count, count)], dst_ref=dst.at[:, mine(me), :],
            send_sem=ss.at[d], recv_sem=rs.at[me], device_id=(d, sp), device_id_type=MESH)

    def arrived(src, dst, ss, rs, s):
        return pltpu.make_async_remote_copy(
            src_ref=src.at[pl.ds(window(s, sp) * count, count)], dst_ref=dst.at[:, mine(s), :],
            send_sem=ss.at[s], recv_sem=rs.at[s], device_id=(s, sp), device_id_type=MESH)

    @pl.loop(1, n)
    def _(k):
        fwd(prior, xb, xs, xr, partner(k)).start()

    keep(prior, xb)
    for load in loads[1:]:
        load.wait()
    by_patch(rawp, pert)
    keep(pert, pb)

    zero = jnp.zeros((LEV, hid), BF16)
    half = (w_in[...].astype(F32) * 0.5).astype(BF16)
    w1[:LEV, :hid] = half
    w1[:LEV, hid:] = zero
    w1[LEV:, :hid] = zero
    w1[LEV:, hid:] = half
    w2[:LEV, :hid] = w_out[...]
    w2[:LEV, hid:] = zero
    w2[LEV:, :hid] = zero
    w2[LEV:, hid:] = w_out[...]
    gain2 = jnp.concatenate([gain[...], gain[...]], axis=1)
    bi = b_in[...] * 0.5
    bi2 = jnp.concatenate([bi, bi], axis=1)
    bo2 = jnp.concatenate([b_out[...], b_out[...]], axis=1)
    ri = lax.broadcasted_iota(jnp.int32, (width, width), 0)
    ci = lax.broadcasted_iota(jnp.int32, (width, width), 1)
    ones = jnp.where((ri < LEV) == (ci < LEV), 1.0 / LEV, 0.0).astype(BF16)
    hots = [jnp.where(slot[pl.ds(first + c, 1), :] == ri, 1.0, 0.0).astype(BF16) for c in range(count)]
    roots = [lax.rsqrt(var[pl.ds(first + c, 1), :]) for c in range(count)]
    near = lax.broadcasted_iota(jnp.int32, (2, span), 1)

    def named(c, side, offset):
        hit = (nbr[...] == lax.rem(sp * span + first + c + offset + total, total)) & (near == first + c)
        return jnp.max(jnp.where(hit, 1.0, 0.0), axis=1, keepdims=True)[side:side + 1, :]

    on_left = [named(c, 0, -1) for c in range(count)]
    on_right = [named(c, 1, 1) for c in range(count)]

    def either(flag, a, b):
        return jnp.where(jnp.broadcast_to(flag, a.shape) > 0.5, a, b)

    def halo(buf, rows, ss, rs, g, side):
        if side == 0:
            return pltpu.make_async_remote_copy(
                src_ref=buf.at[count, rows, :], dst_ref=buf.at[0, rows, :],
                send_sem=ss.at[0, g], recv_sem=rs.at[0, g], device_id=right, device_id_type=MESH)
        return pltpu.make_async_remote_copy(
            src_ref=buf.at[1, rows, :], dst_ref=buf.at[count + 1, rows, :],
            send_sem=ss.at[1, g], recv_sem=rs.at[1, g], device_id=left, device_id_type=MESH)

    def group_rows(g):
        return pl.ds(pl.multiple_of(g * grows, grows), grows)

    @pl.loop(0, groups)
    def _(t):
        g = lax.rem(my_group + t, groups)
        for q in range(gs):
            s = g * gs + q

            @pl.when(s != me)
            def _():
                arrived(prior, xb, xs, xr, s).wait_recv()

        rows = group_rows(g)
        x = xb[:, rows, :].reshape(count * grows, width)
        for _ in range(HOPS):
            hi, lo = split(x * x)
            inv = lax.rsqrt(dot1(hi, ones) + dot1(lo, ones) + 1e-6)
            normed = (x * inv * gain2).astype(BF16)
            h = dot1(normed, w1[...]) + bi2
            hidden = (h + h * jnp.tanh(h)).astype(BF16)
            x = x + lax.dot_general(hidden, w2[...], (((1,), (1,)), ((), ())), preferred_element_type=F32) + bo2
        x = x.reshape(count, grows, width)
        xb[:, rows, :] = x
        for c in range(count):
            hi, lo = split(x[c])
            yb[c + 1, rows, :] = (dot1(hi, hots[c]) + dot1(lo, hots[c])) * roots[c]
        halo(yb, rows, ys, yr, g, 0).start()
        halo(yb, rows, ys, yr, g, 1).start()

    @pl.loop(1, n)
    def _(k):
        fwd(pert, pb, ps, pr, partner(k)).start()

    w = width
    eye = jnp.where(ri == ci, 1.0, 0.0)

    def anomaly(v):
        return split(v - jnp.mean(v, axis=0, keepdims=True))

    def products(i, right_sides):
        hi, lo = obs[i]
        hi, lo = hi.T, lo.T
        rh = jnp.concatenate([r[0] for r in right_sides], axis=1)
        rl = jnp.concatenate([r[1] for r in right_sides], axis=1)
        full = (dot1(hi, rh) + dot1(hi, rl) + dot1(lo, rh)) * (1.0 / (size - 1))
        return [full[:, k * w:(k + 1) * w] for k in range(len(right_sides))]

    obs = {c + 1: anomaly(yb[c + 1]) for c in range(count)}
    states = [anomaly(xb[c]) for c in range(count)]
    yy, yx = {}, {}

    def multiply(i, js, cs):
        if js or cs:
            parts = products(i, [obs[j] for j in js] + [states[c] for c in cs])
            for j in js:
                yy[i, j] = parts.pop(0)
            for c in cs:
                yx[i, c] = parts.pop(0)

    last_one = count + 1
    for i in range(1, count + 1):
        multiply(i, [j for j in range(i, min(i + 2, count) + 1)], [c for c in range(count) if abs(c + 1 - i) < 2])

    @pl.loop(0, groups)
    def _(g):
        for side in range(2):
            halo(yb, group_rows(g), ys, yr, g, side).wait_recv()

    obs[0] = anomaly(yb[0])
    obs[last_one] = anomaly(yb[last_one])
    multiply(0, [j for j in range(0, min(2, last_one) + 1)], [0])
    for i in range(max(1, last_one - 2), last_one):
        multiply(i, [last_one], [])
    multiply(last_one, [last_one], [count - 1])

    s11, s12, s22, g1, g2 = [], [], [], [], []
    for c in range(count):
        e = c + 1
        s11.append(either(on_left[c], yy[e - 1, e - 1], yy[e, e]) + eye)
        s22.append(either(on_right[c], yy[e + 1, e + 1], yy[e, e]) + eye)
        s12.append(either(on_left[c], either(on_right[c], yy[e - 1, e + 1], yy[e - 1, e]), yy[e, e + 1]))
        g1.append(either(on_left[c], yx[e - 1, c], yx[e, c]))
        g2.append(either(on_right[c], yx[e + 1, c], yx[e, c]))
    s21 = [m.T for m in s12]

    def innovate(start, stop):
        @pl.loop(start, stop)
        def _(t):
            g = lax.rem(my_group + t, groups)
            for q in range(gs):
                s = g * gs + q

                @pl.when(s != me)
                def _():
                    arrived(pert, pb, ps, pr, s).wait_recv()

            rows = group_rows(g)
            for c in range(count):
                ib[c + 1, rows, :] = pb[c, rows, :] * roots[c] - yb[c + 1, rows, :]
            halo(ib, rows, isd, ir, g, 0).start()
            halo(ib, rows, isd, ir, g, 1).start()

    pinv = inverses(s11)
    innovate(0, 2)
    es = [doth(pinv[c], s12[c]) for c in range(count)]
    ts = [s22[c] - doth(s21[c], es[c]) for c in range(count)]
    fs = [doth(pinv[c], g1[c]) for c in range(count)]
    tinv = inverses(ts)
    innovate(2, groups)
    gains = []
    for c in range(count):
        k2 = doth(tinv[c], g2[c] - doth(s21[c], fs[c]))
        k1 = fs[c] - doth(es[c], k2)
        gains.append(jnp.concatenate([k1, k2], axis=0))

    def back(d):
        return pltpu.make_async_remote_copy(
            src_ref=res.at[:, mine(d), :], dst_ref=out.at[pl.ds(first, count)],
            send_sem=os_.at[d], recv_sem=orr.at[me], device_id=(d, sp), device_id_type=MESH)

    def returned(s):
        return pltpu.make_async_remote_copy(
            src_ref=res.at[:, mine(s), :], dst_ref=out.at[pl.ds(window(s, sp) * count, count)],
            send_sem=os_.at[s], recv_sem=orr.at[s], device_id=(s, sp), device_id_type=MESH)

    gh = [split(m) for m in gains]

    def pick(c, rows):
        mid = ib[c + 1, rows, :]
        return jnp.concatenate(
            [either(on_left[c], ib[c, rows, :], mid), either(on_right[c], ib[c + 2, rows, :], mid)], axis=1)

    @pl.loop(0, groups)
    def _(t):
        g = lax.rem(my_group + groups // 2 + t, groups)
        rows = group_rows(g)
        for side in range(2):
            halo(ib, rows, isd, ir, g, side).wait_recv()
        for c in range(count):
            ih, il = split(pick(c, rows))
            res[c, rows, :] = xb[c, rows, :] + dot1(ih, gh[c][0]) + dot1(ih, gh[c][1]) + dot1(il, gh[c][0])
        for q in range(gs):
            d = g * gs + lax.rem(me + q, gs)

            @pl.when(d != me)
            def _():
                back(d).start()

    last = pltpu.make_async_copy(res.at[:, mine(me), :], out.at[pl.ds(first, count)], loc.at[2])
    last.start()

    @pl.loop(0, groups)
    def _(g):
        for side in range(2):
            halo(yb, group_rows(g), ys, yr, g, side).wait_send()
            halo(ib, group_rows(g), isd, ir, g, side).wait_send()

    last.wait()

    @pl.loop(1, n)
    def _(k):
        d = lax.rem(me + k, n)
        fwd(prior, xb, xs, xr, d).wait_send()
        fwd(pert, pb, ps, pr, d).wait_send()
        back(d).wait_send()
        returned(d).wait_recv()


def body(prior, pert, slot, var, nbr, gain, w_in, b_in, w_out, b_out):
    n = lax.axis_size("mem")
    ns = lax.axis_size("space")
    each, span, width = prior.shape
    count = span // n
    size = each * n
    hid = w_in.shape[1]
    anyw = pl.BlockSpec(memory_space=pl.ANY)
    hbm = pl.BlockSpec(memory_space=pltpu.HBM)
    groups = n // (4 if n % 4 == 0 else 1)
    dma = pltpu.SemaphoreType.DMA
    small = [slot, var, nbr.T, gain[None], w_in, b_in[None], w_out.T, b_out[None]]
    out = pl.pallas_call(
        functools.partial(kernel, n, ns),
        out_shape=jax.ShapeDtypeStruct((span, each, width), F32),
        in_specs=[hbm] * (2 + len(small)),
        out_specs=anyw,
        scratch_shapes=[
            pltpu.VMEM((each * span, width), F32),
            pltpu.VMEM((each * span, width), F32),
            pltpu.VMEM((span, each, width), F32),
            pltpu.VMEM((span, each, width), F32),
            *[pltpu.VMEM(a.shape, a.dtype) for a in small],
            pltpu.VMEM((count, size, width), F32),
            pltpu.VMEM((count, size, width), F32),
            pltpu.VMEM((count + 2, size, width), F32),
            pltpu.VMEM((count + 2, size, width), F32),
            pltpu.VMEM((count, size, width), F32),
            pltpu.VMEM((width, 2 * hid), BF16),
            pltpu.VMEM((width, 2 * hid), BF16),
            dma((n,)), dma((n,)), dma((n,)), dma((n,)),
            dma((2, groups)), dma((2, groups)), dma((2, groups)), dma((2, groups)),
            dma((n,)), dma((n,)), dma((3 + len(small),)),
        ],
        compiler_params=pltpu.CompilerParams(
            collective_id=0, has_side_effects=True, vmem_limit_bytes=67043328),
        name="cycle",
    )(prior.reshape(each * span, width), pert.reshape(each * span, width), *small)
    return jnp.transpose(out, (1, 0, 2))


def solution(mesh):
    in_specs = (
        P("mem", "space", None), P("mem", "space", None),
        P("space", None), P("space", None), P("space", None),
        P(), P(), P(), P(), P(),
    )
    return jax.shard_map(body, mesh=mesh, in_specs=in_specs, out_specs=P("mem", "space", None), check_vma=False)
```

```python
import functools
import jax
import jax.numpy as jnp
from jax import lax
from jax.experimental import pallas as pl
from jax.experimental.pallas import tpu as pltpu
from jax.sharding import PartitionSpec as P

LEV = 64
HOPS = 2
F32 = jnp.float32
BF16 = jnp.bfloat16
MESH = pl.DeviceIdType.MESH
PRIOR_TURNS = (0, 1)
PERT_TURNS = (0, 1)
TURN_AT = {1: 1, 3: 2, 6: 4}
OUT_TURNS = (2, 1)


def dot1(a, b):
    return jnp.dot(a, b, preferred_element_type=F32)


def split(a):
    hi = a.astype(BF16)
    return hi, (a - hi.astype(F32)).astype(BF16)


def doth(a, b):
    return jnp.dot(a, b, preferred_element_type=F32, precision=lax.Precision.HIGHEST)


def spread_row(v, r):
    return jnp.broadcast_to(v[r:r + 1, :], v.shape)

def sweep(p, base, rows, lanes):
    cols = [jnp.broadcast_to(p[:, base + j:base + j + 1], p.shape) for j in range(8)]
    for j in range(0, 8, 2):
        ca, cb = cols[j], cols[j + 1]
        al, be, de = spread_row(ca, j), spread_row(cb, j), spread_row(cb, j + 1)
        inv = 1.0 / (al * de - be * be)
        ra, rb = rows == j, rows == j + 1
        na = jnp.where(ra, -1.0, jnp.where(rb, 0.0, ca))
        nb = jnp.where(rb, -1.0, jnp.where(ra, 0.0, cb))

        def step(v, a, b):
            t = na * (de * a - be * b) + nb * (al * b - be * a)
            return jnp.where(ra | rb, 0.0, v) - t * inv

        for i in range(j + 2, 8):
            cols[i] = step(cols[i], spread_row(cols[i], j), spread_row(cols[i], j + 1))
        la, lb = lanes == base + j, lanes == base + j + 1
        a = jnp.where(la, 1.0, jnp.where(lb, 0.0, spread_row(p, j)))
        b = jnp.where(lb, 1.0, jnp.where(la, 0.0, spread_row(p, j + 1)))
        p = step(jnp.where(la | lb, 0.0, p), a, b)
    return p

def inverses(mats, nb=16, between=None):
    size = mats[0].shape[0]
    rows = lax.broadcasted_iota(jnp.int32, (8, size), 0)
    lanes = lax.broadcasted_iota(jnp.int32, (8, size), 1)
    wide = lax.broadcasted_iota(jnp.int32, (size, size), 1)
    mats = list(mats)
    for lo in range(0, size, nb):
        panels = [[a[lo + q:lo + q + 8] for q in range(0, nb, 8)] for a in mats]
        for q in range(nb // 8):
            base = lo + 8 * q
            here = (lanes >= base) & (lanes < base + 8)
            for m in panels:
                m[q] = sweep(m[q], base, rows, lanes)
            for m in panels:
                for i in range(nb // 8):
                    if i != q:
                        acc = jnp.where(here, 0.0, m[i])
                        for j in range(8):
                            acc = acc - m[i][:, base + j:base + j + 1] * m[q][j:j + 1, :]
                        m[i] = acc
        hole = (wide >= lo) & (wide < lo + nb)
        for k, a in enumerate(mats):
            p = jnp.concatenate(panels[k], axis=0)
            parts = [p]
            if lo: parts.insert(0, jnp.zeros((lo, size), F32))
            if lo + nb < size: parts.append(jnp.zeros((size - lo - nb, size), F32))
            pad = jnp.concatenate(parts, axis=0)
            out = [p]
            if lo:
                t = a[:lo]
                out.insert(0, jnp.where(hole[:lo], 0.0, t) - doth(t, pad))
            if lo + nb < size:
                t = a[lo + nb:]
                out.append(jnp.where(hole[lo + nb:], 0.0, t) - doth(t, pad))
            mats[k] = jnp.concatenate(out, axis=0)
        if between is not None:
            between(lo // nb)
    return mats


def kernel(n, ns, prior_in, pert_in, *refs):
    small_in, refs = refs[:8], refs[8:]
    out, raw, rawp, prior, pert = refs[:5]
    slot, var, nbr, gain, w_in, b_in, w_out, b_out = small = refs[5:13]
    (xb, pb, yb, ib, res, w1, w2,
     xs, xr, ps, pr, ys, yr, isd, ir, os_, orr, loc) = refs[13:]
    me = lax.axis_index("mem")
    sp = lax.axis_index("space")
    count = xb.shape[0]
    size = xb.shape[1]
    width = xb.shape[2]
    each = size // n
    gs = 4 if n % 4 == 0 else 1
    groups = n // gs
    grows = gs * each
    hid = w_in.shape[1]
    span = n * count
    total = span * ns
    my_group = me // gs

    def window(m, p):
        w = m
        if gs == 4:
            z = m // 4
            w = z * 4 + lax.rem(lax.rem(m // 2, 2) + z, 2) * 2 + lax.rem(m, 2)
        return jnp.where(lax.rem(p, 2) == 0, w, n - 1 - w)

    def holder(w, p):
        w = jnp.where(lax.rem(p, 2) == 0, w, n - 1 - w)
        if gs == 1:
            return w
        z = w // 4
        return z * 4 + lax.rem(lax.rem(w // 2, 2) + z, 2) * 2 + lax.rem(w, 2)

    win = window(me, sp)
    first = win * count
    rsp = lax.rem(sp + (win + 1) // n, ns)
    lsp = lax.rem(sp + ns - (n - win) // n, ns)
    right = (holder(lax.rem(win + 1, n), rsp), rsp)
    left = (holder(lax.rem(win + n - 1, n), lsp), lsp)

    def facing(t, turns):
        k = lax.rem(turns[0] + groups + turns[1] * t, groups)
        g, bit = 0, 1
        while bit < groups:
            g = g + lax.rem(my_group // bit + k // bit, 2) * bit
            bit *= 2
        return g

    def each_peer(start, stop, turns, act):
        @pl.loop(start * gs, stop * gs)
        def _(i):
            d = facing(i // gs, turns) * gs + lax.rem(me + lax.rem(i, gs), gs)

            @pl.when(d != me)
            def _():
                act(d)

    loads = [pltpu.make_async_copy(prior_in, raw, loc.at[0]), pltpu.make_async_copy(pert_in, rawp, loc.at[1])]
    loads += [pltpu.make_async_copy(a, b, loc.at[3 + i]) for i, (a, b) in enumerate(zip(small_in, small))]
    for load in loads:
        load.start()

    bar = pltpu.get_barrier_semaphore()

    @pl.loop(1, n)
    def _(k):
        pl.semaphore_signal(bar, inc=1, device_id=(lax.rem(me + k, n), sp), device_id_type=MESH)

    pl.semaphore_signal(bar, inc=1, device_id=left, device_id_type=MESH)
    pl.semaphore_signal(bar, inc=1, device_id=right, device_id_type=MESH)

    def mine(i):
        return pl.ds(pl.multiple_of(i * each, each), each)

    def by_patch(src, dst):
        @pl.loop(0, span)
        def _(p):
            for m in range(0, each, 8):
                dst[p, pl.ds(m, 8), :] = src[pl.ds(p + m * span, 8, stride=span), :]

    def keep(src, dst):
        for c in range(count):
            dst[c, mine(me), :] = src[first + c]

    loads[0].wait()
    by_patch(raw, prior)
    pl.semaphore_wait(bar, n + 1)

    def fwd(src, dst, ss, rs, d):
        return pltpu.make_async_remote_copy(
            src_ref=src.at[pl.ds(window(d, sp) * count, count)], dst_ref=dst.at[:, mine(me), :],
            send_sem=ss.at[d], recv_sem=rs.at[me], device_id=(d, sp), device_id_type=MESH)

    def arrived(src, dst, ss, rs, s):
        return pltpu.make_async_remote_copy(
            src_ref=src.at[pl.ds(window(s, sp) * count, count)], dst_ref=dst.at[:, mine(s), :],
            send_sem=ss.at[s], recv_sem=rs.at[s], device_id=(s, sp), device_id_type=MESH)

    def send_pert(start, stop):
        each_peer(start, stop, PERT_TURNS, lambda d: fwd(pert, pb, ps, pr, d).start())

    each_peer(0, groups, PRIOR_TURNS, lambda d: fwd(prior, xb, xs, xr, d).start())
    keep(prior, xb)
    for load in loads[1:]:
        load.wait()
    by_patch(rawp, pert)
    keep(pert, pb)

    zero = jnp.zeros((LEV, hid), BF16)
    half = (w_in[...].astype(F32) * 0.5).astype(BF16)
    w1[:LEV, :hid] = half
    w1[:LEV, hid:] = zero
    w1[LEV:, :hid] = zero
    w1[LEV:, hid:] = half
    w2[:LEV, :hid] = w_out[...]
    w2[:LEV, hid:] = zero
    w2[LEV:, :hid] = zero
    w2[LEV:, hid:] = w_out[...]
    gain2 = jnp.concatenate([gain[...], gain[...]], axis=1)
    bi = b_in[...] * 0.5
    bi2 = jnp.concatenate([bi, bi], axis=1)
    bo2 = jnp.concatenate([b_out[...], b_out[...]], axis=1)
    ri = lax.broadcasted_iota(jnp.int32, (width, width), 0)
    ci = lax.broadcasted_iota(jnp.int32, (width, width), 1)
    ones = jnp.where((ri < LEV) == (ci < LEV), 1.0 / LEV, 0.0).astype(BF16)
    hots = [jnp.where(slot[pl.ds(first + c, 1), :] == ri, 1.0, 0.0).astype(BF16) for c in range(count)]
    roots = [lax.rsqrt(var[pl.ds(first + c, 1), :]) for c in range(count)]
    near = lax.broadcasted_iota(jnp.int32, (2, span), 1)

    def named(c, side, offset):
        hit = (nbr[...] == lax.rem(sp * span + first + c + offset + total, total)) & (near == first + c)
        return jnp.max(jnp.where(hit, 1.0, 0.0), axis=1, keepdims=True)[side:side + 1, :]

    on_left = [named(c, 0, -1) for c in range(count)]
    on_right = [named(c, 1, 1) for c in range(count)]

    def either(flag, a, b):
        return jnp.where(jnp.broadcast_to(flag, a.shape) > 0.5, a, b)

    def halo(buf, rows, ss, rs, g, side):
        if side == 0:
            return pltpu.make_async_remote_copy(
                src_ref=buf.at[count, rows, :], dst_ref=buf.at[0, rows, :],
                send_sem=ss.at[0, g], recv_sem=rs.at[0, g], device_id=right, device_id_type=MESH)
        return pltpu.make_async_remote_copy(
            src_ref=buf.at[1, rows, :], dst_ref=buf.at[count + 1, rows, :],
            send_sem=ss.at[1, g], recv_sem=rs.at[1, g], device_id=left, device_id_type=MESH)

    def group_rows(g):
        return pl.ds(pl.multiple_of(g * grows, grows), grows)

    @pl.loop(0, groups)
    def _(t):
        g = facing(t, PRIOR_TURNS)
        for q in range(gs):
            s = g * gs + q

            @pl.when(s != me)
            def _():
                arrived(prior, xb, xs, xr, s).wait_recv()

        rows = group_rows(g)
        x = xb[:, rows, :].reshape(count * grows, width)
        for _ in range(HOPS):
            hi, lo = split(x * x)
            inv = lax.rsqrt(dot1(hi, ones) + dot1(lo, ones) + 1e-6)
            normed = (x * inv * gain2).astype(BF16)
            h = dot1(normed, w1[...]) + bi2
            hidden = (h + h * jnp.tanh(h)).astype(BF16)
            x = x + lax.dot_general(hidden, w2[...], (((1,), (1,)), ((), ())), preferred_element_type=F32) + bo2
        x = x.reshape(count, grows, width)
        xb[:, rows, :] = x
        for c in range(count):
            hi, lo = split(x[c])
            yb[c + 1, rows, :] = (dot1(hi, hots[c]) + dot1(lo, hots[c])) * roots[c]
        halo(yb, rows, ys, yr, g, 0).start()
        halo(yb, rows, ys, yr, g, 1).start()

    send_pert(0, groups)
    w = width
    eye = jnp.where(ri == ci, 1.0, 0.0)

    def anomaly(v):
        return split(v - jnp.mean(v, axis=0, keepdims=True))

    def products(i, right_sides):
        hi, lo = obs[i]
        hi, lo = hi.T, lo.T
        rh = jnp.concatenate([r[0] for r in right_sides], axis=1)
        rl = jnp.concatenate([r[1] for r in right_sides], axis=1)
        full = (dot1(hi, rh) + dot1(hi, rl) + dot1(lo, rh)) * (1.0 / (size - 1))
        return [full[:, k * w:(k + 1) * w] for k in range(len(right_sides))]

    obs = {c + 1: anomaly(yb[c + 1]) for c in range(count)}
    states = [anomaly(xb[c]) for c in range(count)]
    yy, yx = {}, {}

    def multiply(i, js, cs):
        if js or cs:
            parts = products(i, [obs[j] for j in js] + [states[c] for c in cs])
            for j in js:
                yy[i, j] = parts.pop(0)
            for c in cs:
                yx[i, c] = parts.pop(0)

    last_one = count + 1
    for i in range(1, count + 1):
        multiply(i, range(max(1, i - 2), min(i + 2, count) + 1), [c for c in range(count) if abs(c + 1 - i) < 2])

    pinv = inverses([yy[i, i] + eye for i in range(1, count + 1)])
    both = [on_left[c] * on_right[c] for c in range(count)]
    swap = [c + 2 if c + 1 < count else c for c in range(count)]
    ps1 = [either(both[c], pinv[swap[c] - 1], pinv[c]) for c in range(count)]
    fs = [doth(ps1[c], either(both[c], yx[swap[c], c], yx[c + 1, c])) for c in range(count)]

    @pl.loop(0, groups)
    def _(g):
        for side in range(2):
            halo(yb, group_rows(g), ys, yr, g, side).wait_recv()

    obs[0] = anomaly(yb[0])
    obs[last_one] = anomaly(yb[last_one])
    multiply(0, [0, 1, 2], [0])
    multiply(last_one, [last_one, last_one - 1, last_one - 2], [count - 1])

    def second(c, left_one, right_one):
        if c + 1 < count:
            return either(on_left[c], left_one, right_one)
        return either(on_right[c], right_one, left_one)

    ets, ts, gs2 = [], [], []
    for c in range(count):
        e = c + 1
        far = swap[c]
        near_l, near_r = yy[e - 1, e], yy[e + 1, e]
        if far > e:
            s21 = second(c, either(both[c], yy[e - 1, far], near_l), near_r)
        else:
            s21 = second(c, near_l, either(both[c], yy[e + 1, far], near_r))
        et = doth(s21, ps1[c])
        ets.append(et)
        ts.append(second(c, yy[e - 1, e - 1], yy[e + 1, e + 1]) + eye - lax.dot_general(
            et, s21, (((1,), (1,)), ((), ())), preferred_element_type=F32, precision=lax.Precision.HIGHEST))
        gs2.append(second(c, yx[e - 1, c], yx[e + 1, c]) - doth(s21, fs[c]))

    def innovate(start, stop):
        @pl.loop(start, stop)
        def _(t):
            g = facing(t, PERT_TURNS)
            for q in range(gs):
                s = g * gs + q

                @pl.when(s != me)
                def _():
                    arrived(pert, pb, ps, pr, s).wait_recv()

            rows = group_rows(g)
            for c in range(count):
                ib[c + 1, rows, :] = pb[c, rows, :] * roots[c] - yb[c + 1, rows, :]
            halo(ib, rows, isd, ir, g, 0).start()
            halo(ib, rows, isd, ir, g, 1).start()

    done = [0]

    def innovate_to(quarters):
        stop = groups * quarters // 4
        if stop > done[0]:
            innovate(done[0], stop)
            done[0] = stop

    innovate_to(0)
    tinv = inverses(ts, between=lambda k: innovate_to(TURN_AT.get(k, 0)))
    ks = [doth(tinv[c], gs2[c]) for c in range(count)]
    gains = [jnp.concatenate([fs[c] - doth(ets[c].T, ks[c]), ks[c]], axis=0) for c in range(count)]
    innovate_to(4)

    def back(d):
        return pltpu.make_async_remote_copy(
            src_ref=res.at[:, mine(d), :], dst_ref=out.at[pl.ds(first, count)],
            send_sem=os_.at[d], recv_sem=orr.at[me], device_id=(d, sp), device_id_type=MESH)

    def returned(s):
        return pltpu.make_async_remote_copy(
            src_ref=res.at[:, mine(s), :], dst_ref=out.at[pl.ds(window(s, sp) * count, count)],
            send_sem=os_.at[s], recv_sem=orr.at[s], device_id=(s, sp), device_id_type=MESH)

    gh = [split(m) for m in gains]

    def pick(c, rows):
        near_one = either(both[c], ib[swap[c], rows, :], ib[c + 1, rows, :])
        return jnp.concatenate([near_one, second(c, ib[c, rows, :], ib[c + 2, rows, :])], axis=1)

    @pl.loop(0, groups)
    def _(t):
        g = facing(t, OUT_TURNS)
        rows = group_rows(g)
        for side in range(2):
            halo(ib, rows, isd, ir, g, side).wait_recv()
        for c in range(count):
            ih, il = split(pick(c, rows))
            res[c, rows, :] = xb[c, rows, :] + dot1(ih, gh[c][0]) + dot1(ih, gh[c][1]) + dot1(il, gh[c][0])
        each_peer(t, t + 1, OUT_TURNS, lambda d: back(d).start())

    last = pltpu.make_async_copy(res.at[:, mine(me), :], out.at[pl.ds(first, count)], loc.at[2])
    last.start()

    @pl.loop(0, groups)
    def _(g):
        for side in range(2):
            halo(yb, group_rows(g), ys, yr, g, side).wait_send()
            halo(ib, group_rows(g), isd, ir, g, side).wait_send()

    last.wait()

    @pl.loop(1, n)
    def _(k):
        d = lax.rem(me + k, n)
        fwd(prior, xb, xs, xr, d).wait_send()
        fwd(pert, pb, ps, pr, d).wait_send()
        back(d).wait_send()
        returned(d).wait_recv()


def body(prior, pert, slot, var, nbr, gain, w_in, b_in, w_out, b_out):
    n = lax.axis_size("mem")
    ns = lax.axis_size("space")
    each, span, width = prior.shape
    count = span // n
    size = each * n
    hid = w_in.shape[1]
    anyw = pl.BlockSpec(memory_space=pl.ANY)
    hbm = pl.BlockSpec(memory_space=pltpu.HBM)
    groups = n // (4 if n % 4 == 0 else 1)
    dma = pltpu.SemaphoreType.DMA
    small = [slot, var, nbr.T, gain[None], w_in, b_in[None], w_out.T, b_out[None]]
    out = pl.pallas_call(
        functools.partial(kernel, n, ns),
        out_shape=jax.ShapeDtypeStruct((span, each, width), F32),
        in_specs=[hbm] * (2 + len(small)),
        out_specs=anyw,
        scratch_shapes=[
            pltpu.VMEM((each * span, width), F32),
            pltpu.VMEM((each * span, width), F32),
            pltpu.VMEM((span, each, width), F32),
            pltpu.VMEM((span, each, width), F32),
            *[pltpu.VMEM(a.shape, a.dtype) for a in small],
            pltpu.VMEM((count, size, width), F32),
            pltpu.VMEM((count, size, width), F32),
            pltpu.VMEM((count + 2, size, width), F32),
            pltpu.VMEM((count + 2, size, width), F32),
            pltpu.VMEM((count, size, width), F32),
            pltpu.VMEM((width, 2 * hid), BF16),
            pltpu.VMEM((width, 2 * hid), BF16),
            dma((n,)), dma((n,)), dma((n,)), dma((n,)),
            dma((2, groups)), dma((2, groups)), dma((2, groups)), dma((2, groups)),
            dma((n,)), dma((n,)), dma((3 + len(small),)),
        ],
        compiler_params=pltpu.CompilerParams(
            collective_id=0, has_side_effects=True, vmem_limit_bytes=50331648),
        name="cycle",
    )(*[pltpu.with_memory_space_constraint(v, pltpu.HBM) for v in (
        prior.reshape(each * span, width), pert.reshape(each * span, width), *small)])
    return jnp.transpose(out, (1, 0, 2))


def solution(mesh):
    in_specs = (
        P("mem", "space", None), P("mem", "space", None),
        P("space", None), P("space", None), P("space", None),
        P(), P(), P(), P(), P(),
    )
    return jax.shard_map(body, mesh=mesh, in_specs=in_specs, out_specs=P("mem", "space", None), check_vma=False)
```

```python
import functools
import jax
import jax.numpy as jnp
from jax import lax
from jax.experimental import pallas as pl
from jax.experimental.pallas import tpu as pltpu
from jax.sharding import PartitionSpec as P

LEV = 64
HOPS = 2
F32 = jnp.float32
BF16 = jnp.bfloat16
MESH = pl.DeviceIdType.MESH
PRIOR_TURNS = (0, 1)
PERT_TURNS = (0, 1)
TURN_AT = {0: 1, 2: 2, 6: 4}
OUT_TURNS = (0, 1)


def dot1(a, b):
    return jnp.dot(a, b, preferred_element_type=F32)


def split(a):
    hi = a.astype(BF16)
    return hi, (a - hi.astype(F32)).astype(BF16)


def doth(a, b):
    return jnp.dot(a, b, preferred_element_type=F32, precision=lax.Precision.HIGHEST)


def spread_row(v, r):
    return jnp.broadcast_to(v[r:r + 1, :], v.shape)

def sweep(p, base, rows, lanes):
    cols = [jnp.broadcast_to(p[:, base + j:base + j + 1], p.shape) for j in range(8)]
    for j in range(0, 8, 2):
        ca, cb = cols[j], cols[j + 1]
        al, be, de = spread_row(ca, j), spread_row(cb, j), spread_row(cb, j + 1)
        inv = 1.0 / (al * de - be * be)
        ra, rb = rows == j, rows == j + 1
        na = jnp.where(ra, -1.0, jnp.where(rb, 0.0, ca))
        nb = jnp.where(rb, -1.0, jnp.where(ra, 0.0, cb))

        def step(v, a, b):
            t = na * (de * a - be * b) + nb * (al * b - be * a)
            return jnp.where(ra | rb, 0.0, v) - t * inv

        for i in range(j + 2, 8):
            cols[i] = step(cols[i], spread_row(cols[i], j), spread_row(cols[i], j + 1))
        la, lb = lanes == base + j, lanes == base + j + 1
        a = jnp.where(la, 1.0, jnp.where(lb, 0.0, spread_row(p, j)))
        b = jnp.where(lb, 1.0, jnp.where(la, 0.0, spread_row(p, j + 1)))
        p = step(jnp.where(la | lb, 0.0, p), a, b)
    return p

def inverses(mats, nb=16, between=None):
    size = mats[0].shape[0]
    rows = lax.broadcasted_iota(jnp.int32, (8, size), 0)
    lanes = lax.broadcasted_iota(jnp.int32, (8, size), 1)
    wide = lax.broadcasted_iota(jnp.int32, (size, size), 1)
    mats = list(mats)
    for lo in range(0, size, nb):
        panels = [[a[lo + q:lo + q + 8] for q in range(0, nb, 8)] for a in mats]
        for q in range(nb // 8):
            base = lo + 8 * q
            here = (lanes >= base) & (lanes < base + 8)
            for m in panels:
                m[q] = sweep(m[q], base, rows, lanes)
            for m in panels:
                for i in range(nb // 8):
                    if i != q:
                        acc = jnp.where(here, 0.0, m[i])
                        for j in range(8):
                            acc = acc - m[i][:, base + j:base + j + 1] * m[q][j:j + 1, :]
                        m[i] = acc
        hole = (wide >= lo) & (wide < lo + nb)
        for k, a in enumerate(mats):
            p = jnp.concatenate(panels[k], axis=0)
            parts = [p]
            if lo: parts.insert(0, jnp.zeros((lo, size), F32))
            if lo + nb < size: parts.append(jnp.zeros((size - lo - nb, size), F32))
            pad = jnp.concatenate(parts, axis=0)
            out = [p]
            if lo:
                t = a[:lo]
                out.insert(0, jnp.where(hole[:lo], 0.0, t) - doth(t, pad))
            if lo + nb < size:
                t = a[lo + nb:]
                out.append(jnp.where(hole[lo + nb:], 0.0, t) - doth(t, pad))
            mats[k] = jnp.concatenate(out, axis=0)
        if between is not None:
            between(lo // nb)
    return mats


def kernel(n, ns, prior_in, pert_in, *refs):
    small_in, refs = refs[:8], refs[8:]
    out, raw, rawp, prior, pert = refs[:5]
    slot, var, nbr, gain, w_in, b_in, w_out, b_out = small = refs[5:13]
    (xb, pb, yb, ib, res, w1, w2,
     xs, xr, ps, pr, ys, yr, isd, ir, os_, orr, loc) = refs[13:]
    me = lax.axis_index("mem")
    sp = lax.axis_index("space")
    count = xb.shape[0]
    size = xb.shape[1]
    width = xb.shape[2]
    each = size // n
    gs = 4 if n % 4 == 0 else 1
    groups = n // gs
    grows = gs * each
    hid = w_in.shape[1]
    span = n * count
    total = span * ns
    my_group = me // gs

    def window(m, p):
        w = m
        if gs == 4:
            z = m // 4
            w = z * 4 + lax.rem(lax.rem(m // 2, 2) + z, 2) * 2 + lax.rem(m, 2)
        return jnp.where(lax.rem(p, 2) == 0, w, n - 1 - w)

    def holder(w, p):
        w = jnp.where(lax.rem(p, 2) == 0, w, n - 1 - w)
        if gs == 1:
            return w
        z = w // 4
        return z * 4 + lax.rem(lax.rem(w // 2, 2) + z, 2) * 2 + lax.rem(w, 2)

    win = window(me, sp)
    first = win * count
    rsp = lax.rem(sp + (win + 1) // n, ns)
    lsp = lax.rem(sp + ns - (n - win) // n, ns)
    right = (holder(lax.rem(win + 1, n), rsp), rsp)
    left = (holder(lax.rem(win + n - 1, n), lsp), lsp)

    def facing(t, turns):
        k = lax.rem(turns[0] + groups + turns[1] * t, groups)
        g, bit = 0, 1
        while bit < groups:
            g = g + lax.rem(my_group // bit + k // bit, 2) * bit
            bit *= 2
        return g

    def each_peer(start, stop, turns, act):
        @pl.loop(start * gs, stop * gs)
        def _(i):
            d = facing(i // gs, turns) * gs + lax.rem(me + lax.rem(i, gs), gs)

            @pl.when(d != me)
            def _():
                act(d)

    loads = [pltpu.make_async_copy(prior_in, raw, loc.at[0]), pltpu.make_async_copy(pert_in, rawp, loc.at[1])]
    loads += [pltpu.make_async_copy(a, b, loc.at[3 + i]) for i, (a, b) in enumerate(zip(small_in, small))]
    for load in loads:
        load.start()

    bar = pltpu.get_barrier_semaphore()

    @pl.loop(1, n)
    def _(k):
        pl.semaphore_signal(bar, inc=1, device_id=(lax.rem(me + k, n), sp), device_id_type=MESH)

    pl.semaphore_signal(bar, inc=1, device_id=left, device_id_type=MESH)
    pl.semaphore_signal(bar, inc=1, device_id=right, device_id_type=MESH)

    def mine(i):
        return pl.ds(pl.multiple_of(i * each, each), each)

    def by_patch(src, dst):
        @pl.loop(0, span)
        def _(p):
            for m in range(0, each, 8):
                dst[p, pl.ds(m, 8), :] = src[pl.ds(p + m * span, 8, stride=span), :]

    def keep(src, dst):
        for c in range(count):
            dst[c, mine(me), :] = src[first + c]

    loads[0].wait()
    by_patch(raw, prior)
    pl.semaphore_wait(bar, n + 1)

    def fwd(src, dst, ss, rs, d):
        return pltpu.make_async_remote_copy(
            src_ref=src.at[pl.ds(window(d, sp) * count, count)], dst_ref=dst.at[:, mine(me), :],
            send_sem=ss.at[d], recv_sem=rs.at[me], device_id=(d, sp), device_id_type=MESH)

    def arrived(src, dst, ss, rs, s):
        return pltpu.make_async_remote_copy(
            src_ref=src.at[pl.ds(window(s, sp) * count, count)], dst_ref=dst.at[:, mine(s), :],
            send_sem=ss.at[s], recv_sem=rs.at[s], device_id=(s, sp), device_id_type=MESH)

    def send_pert(start, stop):
        @pl.loop(0, n)
        def _(i):
            k = i // 2 // gs + lax.rem(i, 2) * (groups // 2)
            d = facing(k, PERT_TURNS) * gs + lax.rem(me + lax.rem(i // 2, gs), gs)

            @pl.when(d != me)
            def _():
                fwd(pert, pb, ps, pr, d).start()

    each_peer(0, groups, PRIOR_TURNS, lambda d: fwd(prior, xb, xs, xr, d).start())
    keep(prior, xb)
    for load in loads[1:]:
        load.wait()
    by_patch(rawp, pert)
    keep(pert, pb)

    zero = jnp.zeros((LEV, hid), BF16)
    half = (w_in[...].astype(F32) * 0.5).astype(BF16)
    w1[:LEV, :hid] = half
    w1[:LEV, hid:] = zero
    w1[LEV:, :hid] = zero
    w1[LEV:, hid:] = half
    w2[:LEV, :hid] = w_out[...]
    w2[:LEV, hid:] = zero
    w2[LEV:, :hid] = zero
    w2[LEV:, hid:] = w_out[...]
    gain2 = jnp.concatenate([gain[...], gain[...]], axis=1)
    bi = b_in[...] * 0.5
    bi2 = jnp.concatenate([bi, bi], axis=1)
    bo2 = jnp.concatenate([b_out[...], b_out[...]], axis=1)
    ri = lax.broadcasted_iota(jnp.int32, (width, width), 0)
    ci = lax.broadcasted_iota(jnp.int32, (width, width), 1)
    ones = jnp.where((ri < LEV) == (ci < LEV), 1.0 / LEV, 0.0).astype(BF16)
    hots = [jnp.where(slot[pl.ds(first + c, 1), :] == ri, 1.0, 0.0).astype(BF16) for c in range(count)]
    roots = [lax.rsqrt(var[pl.ds(first + c, 1), :]) for c in range(count)]
    near = lax.broadcasted_iota(jnp.int32, (2, span), 1)

    def named(c, side, offset):
        hit = (nbr[...] == lax.rem(sp * span + first + c + offset + total, total)) & (near == first + c)
        return jnp.max(jnp.where(hit, 1.0, 0.0), axis=1, keepdims=True)[side:side + 1, :]

    on_left = [named(c, 0, -1) for c in range(count)]
    on_right = [named(c, 1, 1) for c in range(count)]

    def either(flag, a, b):
        return jnp.where(jnp.broadcast_to(flag, a.shape) > 0.5, a, b)

    def halo(buf, rows, ss, rs, g, side):
        if side == 0:
            return pltpu.make_async_remote_copy(
                src_ref=buf.at[count, rows, :], dst_ref=buf.at[0, rows, :],
                send_sem=ss.at[0, g], recv_sem=rs.at[0, g], device_id=right, device_id_type=MESH)
        return pltpu.make_async_remote_copy(
            src_ref=buf.at[1, rows, :], dst_ref=buf.at[count + 1, rows, :],
            send_sem=ss.at[1, g], recv_sem=rs.at[1, g], device_id=left, device_id_type=MESH)

    def group_rows(g):
        return pl.ds(pl.multiple_of(g * grows, grows), grows)

    @pl.loop(0, groups)
    def _(t):
        g = facing(t, PRIOR_TURNS)
        for q in range(gs):
            s = g * gs + q

            @pl.when(s != me)
            def _():
                arrived(prior, xb, xs, xr, s).wait_recv()

        rows = group_rows(g)
        x = xb[:, rows, :].reshape(count * grows, width)
        for _ in range(HOPS):
            hi, lo = split(x * x)
            inv = lax.rsqrt(dot1(hi, ones) + dot1(lo, ones) + 1e-6)
            normed = (x * inv * gain2).astype(BF16)
            h = dot1(normed, w1[...]) + bi2
            hidden = (h + h * jnp.tanh(h)).astype(BF16)
            x = x + lax.dot_general(hidden, w2[...], (((1,), (1,)), ((), ())), preferred_element_type=F32) + bo2
        x = x.reshape(count, grows, width)
        xb[:, rows, :] = x
        for c in range(count):
            hi, lo = split(x[c])
            yb[c + 1, rows, :] = (dot1(hi, hots[c]) + dot1(lo, hots[c])) * roots[c]
        halo(yb, rows, ys, yr, g, 0).start()
        halo(yb, rows, ys, yr, g, 1).start()

    send_pert(0, groups)
    w = width
    eye = jnp.where(ri == ci, 1.0, 0.0)

    def anomaly(v):
        return split(v - jnp.mean(v, axis=0, keepdims=True))

    def products(i, right_sides):
        hi, lo = obs[i]
        hi, lo = hi.T, lo.T
        rh = jnp.concatenate([r[0] for r in right_sides], axis=1)
        rl = jnp.concatenate([r[1] for r in right_sides], axis=1)
        full = (dot1(hi, rh) + dot1(hi, rl) + dot1(lo, rh)) * (1.0 / (size - 1))
        return [full[:, k * w:(k + 1) * w] for k in range(len(right_sides))]

    obs = {c + 1: anomaly(yb[c + 1]) for c in range(count)}
    states = [anomaly(xb[c]) for c in range(count)]
    yy, yx = {}, {}

    def multiply(i, js, cs):
        if js or cs:
            parts = products(i, [obs[j] for j in js] + [states[c] for c in cs])
            for j in js:
                yy[i, j] = parts.pop(0)
            for c in cs:
                yx[i, c] = parts.pop(0)

    last_one = count + 1
    for i in range(1, count + 1):
        multiply(i, range(max(1, i - 2), min(i + 2, count) + 1), [c for c in range(count) if abs(c + 1 - i) < 2])

    pinv = inverses([yy[i, i] + eye for i in range(1, count + 1)])
    both = [on_left[c] * on_right[c] for c in range(count)]
    swap = [c + 2 if c + 1 < count else c for c in range(count)]
    ps1 = [either(both[c], pinv[swap[c] - 1], pinv[c]) for c in range(count)]
    fs = [doth(ps1[c], either(both[c], yx[swap[c], c], yx[c + 1, c])) for c in range(count)]

    @pl.loop(0, groups)
    def _(g):
        for side in range(2):
            halo(yb, group_rows(g), ys, yr, g, side).wait_recv()

    obs[0] = anomaly(yb[0])
    obs[last_one] = anomaly(yb[last_one])
    multiply(0, [0, 1, 2], [0])
    multiply(last_one, [last_one, last_one - 1, last_one - 2], [count - 1])

    def second(c, left_one, right_one):
        if c + 1 < count:
            return either(on_left[c], left_one, right_one)
        return either(on_right[c], right_one, left_one)

    ets, ts, gs2 = [], [], []
    for c in range(count):
        e = c + 1
        far = swap[c]
        near_l, near_r = yy[e - 1, e], yy[e + 1, e]
        if far > e:
            s21 = second(c, either(both[c], yy[e - 1, far], near_l), near_r)
        else:
            s21 = second(c, near_l, either(both[c], yy[e + 1, far], near_r))
        et = doth(s21, ps1[c])
        ets.append(et)
        ts.append(second(c, yy[e - 1, e - 1], yy[e + 1, e + 1]) + eye - lax.dot_general(
            et, s21, (((1,), (1,)), ((), ())), preferred_element_type=F32, precision=lax.Precision.HIGHEST))
        gs2.append(second(c, yx[e - 1, c], yx[e + 1, c]) - doth(s21, fs[c]))

    def innovate(start, stop):
        @pl.loop(start, stop)
        def _(t):
            g = facing(t // 2 + lax.rem(t, 2) * (groups // 2), PERT_TURNS)
            for q in range(gs):
                s = g * gs + q

                @pl.when(s != me)
                def _():
                    arrived(pert, pb, ps, pr, s).wait_recv()

            rows = group_rows(g)
            for c in range(count):
                ib[c + 1, rows, :] = pb[c, rows, :] * roots[c] - yb[c + 1, rows, :]
            halo(ib, rows, isd, ir, g, 0).start()
            halo(ib, rows, isd, ir, g, 1).start()

    done = [0]

    def innovate_to(quarters):
        stop = groups * quarters // 4
        if stop > done[0]:
            innovate(done[0], stop)
            done[0] = stop

    innovate_to(0)
    tinv = inverses(ts, between=lambda k: innovate_to(TURN_AT.get(k, 0)))
    ks = [doth(tinv[c], gs2[c]) for c in range(count)]
    gains = [jnp.concatenate([fs[c] - doth(ets[c].T, ks[c]), ks[c]], axis=0) for c in range(count)]
    innovate_to(4)

    def back(d):
        return pltpu.make_async_remote_copy(
            src_ref=res.at[:, mine(d), :], dst_ref=out.at[pl.ds(first, count)],
            send_sem=os_.at[d], recv_sem=orr.at[me], device_id=(d, sp), device_id_type=MESH)

    def returned(s):
        return pltpu.make_async_remote_copy(
            src_ref=res.at[:, mine(s), :], dst_ref=out.at[pl.ds(window(s, sp) * count, count)],
            send_sem=os_.at[s], recv_sem=orr.at[s], device_id=(s, sp), device_id_type=MESH)

    gh = [split(m) for m in gains]

    def pick(c, rows):
        near_one = either(both[c], ib[swap[c], rows, :], ib[c + 1, rows, :])
        return jnp.concatenate([near_one, second(c, ib[c, rows, :], ib[c + 2, rows, :])], axis=1)

    @pl.loop(0, groups)
    def _(t):
        g = facing(t // 2 + lax.rem(t + 1, 2) * (groups // 2), OUT_TURNS)
        rows = group_rows(g)
        for side in range(2):
            halo(ib, rows, isd, ir, g, side).wait_recv()
        for c in range(count):
            ih, il = split(pick(c, rows))
            res[c, rows, :] = xb[c, rows, :] + dot1(ih, gh[c][0]) + dot1(ih, gh[c][1]) + dot1(il, gh[c][0])
        for q in range(gs):
            d = g * gs + lax.rem(me + q, gs)

            @pl.when(d != me)
            def _():
                back(d).start()

    last = pltpu.make_async_copy(res.at[:, mine(me), :], out.at[pl.ds(first, count)], loc.at[2])
    last.start()

    @pl.loop(0, groups)
    def _(g):
        for side in range(2):
            halo(yb, group_rows(g), ys, yr, g, side).wait_send()
            halo(ib, group_rows(g), isd, ir, g, side).wait_send()

    last.wait()

    @pl.loop(1, n)
    def _(k):
        d = lax.rem(me + k, n)
        fwd(prior, xb, xs, xr, d).wait_send()
        fwd(pert, pb, ps, pr, d).wait_send()
        back(d).wait_send()
        returned(d).wait_recv()


def body(prior, pert, slot, var, nbr, gain, w_in, b_in, w_out, b_out):
    n = lax.axis_size("mem")
    ns = lax.axis_size("space")
    each, span, width = prior.shape
    count = span // n
    size = each * n
    hid = w_in.shape[1]
    anyw = pl.BlockSpec(memory_space=pl.ANY)
    hbm = pl.BlockSpec(memory_space=pltpu.HBM)
    groups = n // (4 if n % 4 == 0 else 1)
    dma = pltpu.SemaphoreType.DMA
    small = [slot, var, nbr.T, gain[None], w_in, b_in[None], w_out.T, b_out[None]]
    out = pl.pallas_call(
        functools.partial(kernel, n, ns),
        out_shape=jax.ShapeDtypeStruct((span, each, width), F32),
        in_specs=[hbm] * (2 + len(small)),
        out_specs=anyw,
        scratch_shapes=[
            pltpu.VMEM((each * span, width), F32),
            pltpu.VMEM((each * span, width), F32),
            pltpu.VMEM((span, each, width), F32),
            pltpu.VMEM((span, each, width), F32),
            *[pltpu.VMEM(a.shape, a.dtype) for a in small],
            pltpu.VMEM((count, size, width), F32),
            pltpu.VMEM((count, size, width), F32),
            pltpu.VMEM((count + 2, size, width), F32),
            pltpu.VMEM((count + 2, size, width), F32),
            pltpu.VMEM((count, size, width), F32),
            pltpu.VMEM((width, 2 * hid), BF16),
            pltpu.VMEM((width, 2 * hid), BF16),
            dma((n,)), dma((n,)), dma((n,)), dma((n,)),
            dma((2, groups)), dma((2, groups)), dma((2, groups)), dma((2, groups)),
            dma((n,)), dma((n,)), dma((3 + len(small),)),
        ],
        compiler_params=pltpu.CompilerParams(
            collective_id=0, has_side_effects=True, vmem_limit_bytes=50331648),
        name="cycle",
    )(*[pltpu.with_memory_space_constraint(v, pltpu.HBM) for v in (
        prior.reshape(each * span, width), pert.reshape(each * span, width), *small)])
    return jnp.transpose(out, (1, 0, 2))


def solution(mesh):
    in_specs = (
        P("mem", "space", None), P("mem", "space", None),
        P("space", None), P("space", None), P("space", None),
        P(), P(), P(), P(), P(),
    )
    return jax.shard_map(body, mesh=mesh, in_specs=in_specs, out_specs=P("mem", "space", None), check_vma=False)
```
